1024 devices in a mesh: dp: 32 (over x, z_hi, core), expert: 32 (over z_lo, y).
Axes of the slice: x: 4, y: 4, z: 32 (z_hi: 4, z_lo: 8; z = z_hi * 8 + z_lo), core: 2. Of those that a mesh axis runs over, the one named last changes fastest.
Arguments:
- tokens: bfloat16 [131072, 2560], P(('dp', 'expert')), parts along dimension 0, may hold values from -6 to 6
- expert_ids: int32 [131072, 2], P(('dp', 'expert')), parts along dimension 0, may hold values from 0 to 15, all different within a row; in each aligned block of 128 rows (0 to 127, 128 to 255, ...) at most 20 rows name the same one
- gate_weights: float32 [131072, 2], P(('dp', 'expert')), parts along dimension 0, may hold values from 0.1 to 1
- w_gate: bfloat16 [2560, 12288], P(None, 'expert'), may hold values from -0.125 to 0.125
- w_up: bfloat16 [2560, 12288], P(None, 'expert'), may hold values from -0.125 to 0.125
- w_down: bfloat16 [12288, 2560], P('expert'), may hold values from -0.21875 to 0.21875
Outputs:
- moe_out: bfloat16 [131072, 2560], P(('dp', 'expert')), parts along dimension 0
The draws below stay inside these ranges and needn't reach their ends.
There are 32 independent parts, one for each index of `dp`. The reference program is written for one: setup_inputs(seed, part) draws one part's arguments, and reference() takes and returns one part's arrays. A program takes and returns all parts, laid end to end along the dimension named above; an argument that names none is the same for every part. Nothing has to cross between parts.
Inputs may be any that keep to these rules, and one draw needn't show every extreme that they name: `expert_ids`: each row names 2 different experts; in each aligned block of 128 rows (the rows of one device) no expert is named by more than 20 rows, a bound that some block reaches.
All inputs are finite; a program needn't handle non-finite values.
Results may differ from the reference program's by a relative error of at most 0.01.
Values may be sent and summed in bfloat16 or wider, within the bound.
No kernel may reach another device: no remote copies, remote signals or barrier semaphores. Data moves between devices by JAX's collectives and lax.ppermute only.
A program may use at most 64 MiB of HBM per device.

```python
import math
import jax
import jax.numpy as jnp
import numpy as np
from jax import lax

D = 2560
FF = 768
EXPERTS = 16
TOPK = 2
TOK_DEV = 128
CAP = 20
TOKENS = 4096
SPLIT = 2
HID_BLOCK = 384
N_EXPERT = 32


def level_of(rng, extent, cuts, least, high):
    level = 1.0
    for dim, parts in cuts:
        steps = jax.random.uniform(jax.random.fold_in(jax.random.fold_in(rng, 6), dim), (parts,), jnp.float32, least / len(cuts), high / len(cuts))
        level = level * jnp.repeat(jnp.exp(steps), extent[dim] // parts).reshape((-1,) + (1,) * (len(extent) - 1 - dim))
    return level


def assign_block(rng, own, number, rows, amount, top, most, skew):
    order = jax.random.permutation(rng, amount)
    crowded, common = shares(amount, rows * top, most, skew, True), shares(amount, rows * top, most, skew, False)
    places = jnp.arange(amount)

    def named(tallies, turn):
        used = int((tallies > 0).sum())
        fixed = max(1, used // 4)
        shifted = fixed + (places - fixed + turn * (used - fixed)) % max(1, amount - fixed)
        return jnp.zeros((amount,), jnp.int32).at[order[jnp.where(places < fixed, places, shifted)]].set(jnp.asarray(tallies, jnp.int32))

    tallies = jnp.where(number % 4 == 0, named(crowded, number // 4), named(common, number - number // 4 - 1))
    mixed = jax.random.permutation(jax.random.fold_in(own, 3), amount)
    donor, taker = mixed[0:amount // 2 * 2:2], mixed[1:amount // 2 * 2:2]
    slack = jnp.minimum(tallies[donor] - 1, most - tallies[taker]) // 2
    slack = jnp.where((donor == order[0]) | (taker == order[0]) | (tallies[taker] == 0), 0, jnp.maximum(slack, 0))
    shifted = jax.random.randint(jax.random.fold_in(own, 4), (amount // 2,), 0, 1 << 20) % (slack + 1)
    tallies = tallies.at[donor].add(-shifted).at[taker].add(shifted)
    items = jnp.searchsorted(jnp.cumsum(tallies), jnp.arange(rows * top), side="right").astype(jnp.int32)
    listing = items.reshape(top, rows).T
    listing = listing[jax.random.permutation(jax.random.fold_in(own, 1), rows)]
    turn = jax.random.randint(jax.random.fold_in(own, 2), (rows, 1), 0, top)
    return jnp.take_along_axis(listing, (jnp.arange(top)[None, :] + turn) % top, axis=1)


def shares(number_of, total, bound, lean, full):
    portions = [(1 << 20) // math.isqrt(standing ** lean) + 1 for standing in range(1, number_of + 1)]
    largest = bound if full else min(bound, max(-(-total // number_of), total * portions[0] // sum(portions)))
    least = 1 if total - largest >= number_of - 1 else 0
    counts, surplus = [largest] + [least] * (number_of - 1), total - largest - least * (number_of - 1)
    while surplus > 0:
        movable = [i for i in range(1, number_of) if counts[i] < largest] or [i for i in range(1, number_of) if counts[i] < bound]
        whole, budget = sum([portions[i] for i in movable]), surplus
        for i in movable:
            addition = min(bound - counts[i], max(1, budget * portions[i] // whole), surplus)
            counts[i] = counts[i] + addition
            surplus = surplus - addition
    return np.array(counts)


def scatter_about(stream_key, dims, scale, bound, split=(), held_as=jnp.bfloat16):
    array = jax.random.normal(stream_key, dims, jnp.float32) * scale
    if len(split) > 0:
        array = level_of(stream_key, dims, split, -0.22, 0.18) * array
    return jnp.clip(array, min=-bound, max=bound).astype(held_as)


def setup_inputs(seed: int = 0, part: int = 0) -> dict:
    arg_keys = jax.random.split(jax.random.key(seed), 7)
    part_splits = jax.random.split(jax.random.fold_in(arg_keys[6], part), 7)
    tokens = scatter_about(part_splits[0], (TOKENS, D), 1.0, 6.0, ((0, 32),))
    expert_ids_keys = jax.random.split(jax.random.fold_in(part_splits[1], 1), TOKENS // TOK_DEV)
    expert_ids_turns = jax.random.permutation(jax.random.fold_in(part_splits[1], 3), TOKENS // TOK_DEV)
    expert_ids = jax.vmap(lambda own, number: assign_block(jax.random.fold_in(part_splits[1], 2), own, number, TOK_DEV, EXPERTS, TOPK, CAP, 2))(expert_ids_keys, expert_ids_turns).reshape((TOKENS, TOPK))
    gate_weights = jnp.clip(jnp.exp(math.log(1.0) - 2.3025851 * jax.random.uniform(part_splits[2], (TOKENS, TOPK), jnp.float32) ** level_of(part_splits[2], (TOKENS, TOPK), ((0, 32),), -0.2, 0.2)), 0.1, 1.0)
    w_gate = scatter_about(arg_keys[3], (D, EXPERTS * FF), D ** -0.5, 0.125, ((1, 32),))
    w_up = scatter_about(arg_keys[4], (D, EXPERTS * FF), D ** -0.5, 0.125, ((1, 32),))
    w_down = scatter_about(arg_keys[5], (EXPERTS * FF, D), FF ** -0.5, 0.21875, ((0, 32),))
    return {"tokens": tokens, "expert_ids": expert_ids, "gate_weights": gate_weights, "w_gate": w_gate, "w_up": w_up, "w_down": w_down}


def slot_places(source_ids):
    one_hot = (source_ids[..., None] == jnp.arange(EXPERTS, dtype=jnp.int32)).astype(jnp.int32)
    earlier = jnp.cumsum(one_hot, axis=-2) - one_hot
    return jnp.sum(earlier * one_hot, axis=-1).astype(jnp.int32)


def expert_block(operands):
    block_rows, gate_cols, up_cols, down_rows = operands
    gate_act = jnp.dot(block_rows, gate_cols, preferred_element_type=jnp.float32)
    up_act = jnp.dot(block_rows, up_cols, preferred_element_type=jnp.float32)
    hidden = (jax.nn.silu(gate_act) * up_act).astype(jnp.bfloat16)
    summed = jnp.zeros((block_rows.shape[0], down_rows.shape[1]), jnp.float32)
    for member in range(SPLIT):
        lower_col = member * HID_BLOCK
        partial_sum = jnp.dot(hidden[:, lower_col:lower_col + HID_BLOCK], down_rows[lower_col:lower_col + HID_BLOCK], preferred_element_type=jnp.float32).astype(jnp.bfloat16)
        summed = summed + partial_sum.astype(jnp.float32)
    return summed.astype(jnp.bfloat16)


def reference(tokens, expert_ids, gate_weights, w_gate, w_up, w_down):
    source_ids = expert_ids.reshape(N_EXPERT, TOK_DEV * TOPK)
    slot_index = slot_places(source_ids)
    sources = jnp.arange(N_EXPERT, dtype=jnp.int32)[:, None]
    position = ((source_ids * N_EXPERT + sources) * CAP + slot_index).reshape(-1).astype(jnp.int32)
    token_of = (jnp.arange(TOKENS * TOPK, dtype=jnp.int32) // TOPK).astype(jnp.int32)
    buffer = jnp.zeros((EXPERTS * N_EXPERT * CAP, D), tokens.dtype).at[position].set(tokens[token_of])
    gate_stack = w_gate.reshape(D, EXPERTS, FF).transpose(1, 0, 2)
    up_stack = w_up.reshape(D, EXPERTS, FF).transpose(1, 0, 2)
    down_stack = w_down.reshape(EXPERTS, FF, D)
    outputs = lax.map(expert_block, (buffer.reshape(EXPERTS, N_EXPERT * CAP, D), gate_stack, up_stack, down_stack))
    picked = outputs.reshape(-1, D)[position].reshape(TOKENS, TOPK, D).astype(jnp.float32)
    return jnp.sum(picked * gate_weights[:, :, None], axis=1).astype(jnp.bfloat16)
```

```python
import jax
import jax.numpy as jnp
from jax import lax
from jax.experimental import pallas as pl
from jax.experimental.pallas import tpu as pltpu
from jax.sharding import PartitionSpec as P


D = 2560
HID = 384
TOK = 128
CAP = 20
BLK = 2 * CAP
NB = 8
ROWS = NB * BLK
AXES = ("dp", "expert")
VMEM = pl.BlockSpec(memory_space=pltpu.VMEM)
SMEM = pl.BlockSpec(memory_space=pltpu.SMEM)
BLOCKS = (
    ((0, 4), (0, 3), (1, 3), (0, 2), (1, 2), (0, 1), (1, 1), (0, 0)),
    ((1, -4), (1, -3), (0, -3), (1, -2), (0, -2), (1, -1), (0, -1), (1, 0)),
)


def pairs_of(move):
    def index(x, y, z, c):
        return ((x % 4) * 8 + (z % 32) // 8 * 2 + c) * 32 + (z % 8) * 4 + y % 4

    return sorted(
        (index(x, y, z, c), index(*move(x, y, z, c)))
        for x in range(4)
        for y in range(4)
        for z in range(32)
        for c in range(2)
    )


def block_move(k):
    def move(x, y, z, c):
        far, away = BLOCKS[c][k]
        return x, 3 - y if far else y, z + away, c

    return move


def send(value, move, back=False):
    pairs = pairs_of(move)
    if back:
        pairs = sorted((b, a) for a, b in pairs)
    return lax.ppermute(value, AXES, pairs)


def other_core(x, y, z, c):
    return x, y, z, 1 - c


def pair_y(x, y, z, c):
    return x, y ^ 1, z, c


def pair_x(x, y, z, c):
    return x ^ 1, y, z, c


def places(small, experts):
    hit0 = small[0:1, :] == experts
    hit1 = small[1:2, :] == experts
    hit = hit0 | hit1
    src = lax.broadcasted_iota(jnp.int32, (TOK, TOK), 0)
    dst = lax.broadcasted_iota(jnp.int32, (TOK, TOK), 1)
    before = (src < dst).astype(jnp.bfloat16)
    rank = jnp.dot(
        hit.astype(jnp.float32).astype(jnp.bfloat16),
        before,
        preferred_element_type=jnp.float32,
    )
    weight = jnp.where(hit0, small[2:3, :], small[3:4, :])
    return jnp.where(hit, rank, -1.0), weight


def chooser(own, other, experts, weighted):
    own_pos, own_w = places(own[...], experts[...])
    other_pos, other_w = places(other[...], experts[...])
    pos = jnp.concatenate([own_pos, other_pos], axis=1)
    weight = jnp.concatenate([own_w, other_w], axis=1)
    row = lax.broadcasted_iota(jnp.int32, (BLK, 2 * TOK), 0)
    lane = lax.broadcasted_iota(jnp.int32, (BLK, 2 * TOK), 1)
    slot = jnp.where(
        lane < TOK,
        jnp.where(row < CAP, row, -2),
        jnp.where(row >= CAP, row - CAP, -2),
    ).astype(jnp.float32)
    parts = []
    for b in range(NB):
        value = weight[b : b + 1, :] if weighted else 1.0
        parts.append(jnp.where(pos[b : b + 1, :] == slot, value, 0.0))
    return jnp.concatenate(parts, axis=0)


def gather_kernel(own_small, other_small, experts, own_tok, other_tok, *outs):
    choose = chooser(own_small, other_small, experts, False).astype(jnp.bfloat16)
    step = 512
    for lo in range(0, D, step):
        cols = slice(lo, lo + step)
        rows = jnp.dot(
            choose[:, :TOK], own_tok[:, cols], preferred_element_type=jnp.float32
        ) + jnp.dot(
            choose[:, TOK:], other_tok[:, cols], preferred_element_type=jnp.float32
        )
        for b in range(NB):
            outs[b][:, cols] = rows[b * BLK : (b + 1) * BLK].astype(jnp.bfloat16)


def gather(own_small, other_small, experts, own_tok, other_tok):
    return pl.pallas_call(
        gather_kernel,
        out_shape=[jax.ShapeDtypeStruct((BLK, D), jnp.bfloat16)] * NB,
        in_specs=[VMEM] * 5,
        out_specs=[VMEM] * NB,
        name="gather_rows",
    )(own_small, other_small, experts, own_tok, other_tok)


def mixer_kernel(own_small, other_small, experts, high, low):
    mix = chooser(own_small, other_small, experts, True).T
    rounded = mix.astype(jnp.bfloat16)
    high[...] = rounded
    low[...] = (mix - rounded.astype(jnp.float32)).astype(jnp.bfloat16)


def mixer(own_small, other_small, experts):
    return pl.pallas_call(
        mixer_kernel,
        out_shape=[jax.ShapeDtypeStruct((2 * TOK, ROWS), jnp.bfloat16)] * 2,
        in_specs=[VMEM] * 3,
        out_specs=[VMEM] * 2,
        name="mix_matrix",
    )(own_small, other_small, experts)


def join(blocks, rows):
    for b in range(NB):
        rows[b * BLK : (b + 1) * BLK, :] = blocks[b][...]


def act(gate, up):
    return (gate / (1.0 + jnp.exp(-gate)) * up).astype(jnp.bfloat16)


def hidden_own_kernel(w_gate, w_up, *refs):
    blocks, hidden, rows = refs[:NB], refs[NB], refs[NB + 1]
    join(blocks, rows)
    x = rows[...]
    gate = jnp.dot(x, w_gate[...], preferred_element_type=jnp.float32)
    up = jnp.dot(x, w_up[...], preferred_element_type=jnp.float32)
    hidden[...] = act(gate, up)


def hidden_own(w_gate, w_up, blocks):
    return pl.pallas_call(
        hidden_own_kernel,
        out_shape=jax.ShapeDtypeStruct((ROWS, HID), jnp.bfloat16),
        in_specs=[VMEM] * (2 + NB),
        out_specs=VMEM,
        scratch_shapes=[pltpu.VMEM((ROWS, D), jnp.bfloat16)],
        name="hidden_own",
    )(w_gate, w_up, *blocks)


def hidden_other_kernel(starts, *refs):
    pieces, blocks, hidden, rows = refs[:4], refs[4 : 4 + NB], refs[4 + NB], refs[5 + NB]
    join(blocks, rows)
    gate = jnp.zeros((ROWS, HID), jnp.float32)
    up = jnp.zeros((ROWS, HID), jnp.float32)
    for k, piece in enumerate(pieces):
        x = rows[:, pl.ds(pl.multiple_of(starts[k], 128), D // 4)]
        gate = gate + jnp.dot(x, piece[0], preferred_element_type=jnp.float32)
        up = up + jnp.dot(x, piece[1], preferred_element_type=jnp.float32)
    hidden[...] = act(gate, up)


def hidden_other(starts, pieces, blocks):
    return pl.pallas_call(
        hidden_other_kernel,
        out_shape=jax.ShapeDtypeStruct((ROWS, HID), jnp.bfloat16),
        in_specs=[SMEM] + [VMEM] * (4 + NB),
        out_specs=VMEM,
        scratch_shapes=[pltpu.VMEM((ROWS, D), jnp.bfloat16)],
        name="hidden_other",
    )(starts, *pieces, *blocks)


def down_kernel(starts, own_hidden, other_hidden, w_down, *refs):
    pieces, outs = refs[:4], refs[4:]
    for k, piece in enumerate(pieces):
        cols = pl.ds(pl.multiple_of(starts[k], 128), D // 4)
        result = jnp.dot(
            own_hidden[...], w_down[:, cols], preferred_element_type=jnp.float32
        ) + jnp.dot(other_hidden[...], piece[...], preferred_element_type=jnp.float32)
        for b in range(NB):
            outs[b][:, cols] = result[b * BLK : (b + 1) * BLK].astype(jnp.bfloat16)


def down(starts, own_hidden, other_hidden, w_down, pieces):
    return pl.pallas_call(
        down_kernel,
        out_shape=[jax.ShapeDtypeStruct((BLK, D), jnp.bfloat16)] * NB,
        in_specs=[SMEM] + [VMEM] * 7,
        out_specs=[VMEM] * NB,
        name="down_rows",
    )(starts, own_hidden, other_hidden, w_down, *pieces)


def mixed(high, low, part):
    return jnp.dot(high, part, preferred_element_type=jnp.float32) + jnp.dot(
        low, part, preferred_element_type=jnp.float32
    )


def mix_other_kernel(high, low, *refs):
    blocks, other, rows = refs[:NB], refs[NB], refs[NB + 1]
    join(blocks, rows)
    step = 512
    for lo in range(0, D, step):
        cols = slice(lo, lo + step)
        other[:, cols] = mixed(high[TOK:], low[TOK:], rows[:, cols]).astype(
            jnp.bfloat16
        )


def mix_own_kernel(high, low, *refs):
    blocks, own, rows = refs[:NB], refs[NB], refs[NB + 1]
    join(blocks, rows)
    step = 512
    for lo in range(0, D, step):
        cols = slice(lo, lo + step)
        own[:, cols] = mixed(high[:TOK], low[:TOK], rows[:, cols])


def mix(kernel, dtype, high, low, blocks):
    return pl.pallas_call(
        kernel,
        out_shape=jax.ShapeDtypeStruct((TOK, D), dtype),
        in_specs=[VMEM] * (2 + NB),
        out_specs=VMEM,
        scratch_shapes=[pltpu.VMEM((ROWS, D), jnp.bfloat16)],
    )(high, low, *blocks)


def layer(tokens, expert_ids, gate_weights, w_gate, w_up, w_down):
    place, part = lax.axis_index("expert"), lax.axis_index("dp")
    core, x_odd = part % 2, (part // 8) % 2
    z, y = place // 4, place % 4
    far = jnp.where(core == 0, *(jnp.array([f for f, _ in BLOCKS[c]]) for c in range(2)))
    away = jnp.where(core == 0, *(jnp.array([a for _, a in BLOCKS[c]]) for c in range(2)))
    expert = ((z + away + 8) % 8) * 2 + (far ^ (y // 2))
    experts = jnp.broadcast_to(expert.astype(jnp.float32)[:, None], (NB, TOK))
    small = jnp.concatenate(
        [
            expert_ids.T.astype(jnp.float32),
            gate_weights.T,
            jnp.zeros((4, TOK), jnp.float32),
        ]
    )
    other_tok = send(tokens, other_core)
    other_small = send(small, other_core)
    blocks = gather(small, other_small, experts, tokens, other_tok)

    piece = x_odd * 2 + core
    rows_at = piece * (D // 4)
    gate_up = jnp.stack(
        [
            lax.dynamic_slice(w_gate, (rows_at, 0), (D // 4, HID)),
            lax.dynamic_slice(w_up, (rows_at, 0), (D // 4, HID)),
        ]
    )
    down_cols = lax.dynamic_slice(w_down, (0, rows_at), (HID, D // 4))
    gu0 = send(gate_up, pair_y)
    dn0 = send(down_cols, pair_y)
    gu1 = send(gu0, pair_x)
    dn1 = send(dn0, pair_x)
    gu2 = send(gu0, other_core)
    gu3 = send(gu1, other_core)
    dn2 = send(dn0, other_core)
    dn3 = send(dn1, other_core)
    starts = jnp.stack(
        [
            (a * 2 + b) * (D // 4)
            for a, b in (
                (x_odd, core),
                (1 - x_odd, core),
                (x_odd, 1 - core),
                (1 - x_odd, 1 - core),
            )
        ]
    ).astype(jnp.int32)

    arrived = []
    for k in range(NB):
        arrived.append(send(blocks[k], block_move(k)))
    high, low = mixer(small, other_small, experts)
    h_own = hidden_own(w_gate, w_up, arrived)
    h_other = hidden_other(starts, (gu0, gu1, gu2, gu3), arrived)
    results = down(starts, h_own, h_other, w_down, (dn0, dn1, dn2, dn3))
    returned = []
    for k in range(NB):
        returned.append(send(results[k], block_move(k), back=True))
    theirs = mix(mix_other_kernel, jnp.bfloat16, high, low, returned)
    rest = send(theirs, other_core)
    mine = mix(mix_own_kernel, jnp.float32, high, low, returned)
    return (mine + rest.astype(jnp.float32)).astype(jnp.bfloat16)


def solution(mesh):
    in_specs = (
        P(AXES, None),
        P(AXES, None),
        P(AXES, None),
        P(None, "expert"),
        P(None, "expert"),
        P("expert", None),
    )
    return jax.shard_map(
        layer,
        mesh=mesh,
        in_specs=in_specs,
        out_specs=P(AXES, None),
        check_vma=False,
    )
```
